32 devices in a mesh: row: 8 (over z, y), col: 4 (over x, core).
Axes of the slice: x: 2, y: 2, z: 4, core: 2. Of those that a mesh axis runs over, the one named last changes fastest.
Arguments:
- act_quant: bfloat16 [512, 8192], P('row', 'col'), may hold values from -127 to 127, as said below
- act_scale: float32 [512], replicated, may hold values from 0.004 to 0.04
- gate_up_quant: bfloat16 [2, 8192, 29568], P(None, 'col', 'row'), may hold values from -127 to 127, as said below
- gate_up_scale: float32 [2, 29568], P(None, 'row'), may hold values from 5e-05 to 0.0005
- down_quant: bfloat16 [29568, 8192], P('row', 'col'), may hold values from -127 to 127, as said below
- down_scale: float32 [8192], P('col'), may hold values from 3e-05 to 0.0003
Outputs:
- mixed_out: bfloat16 [512, 8192], P('row', 'col')
The draws below stay inside these ranges and needn't reach their ends.
Inputs may be any that keep to these rules, and one draw needn't show every extreme that they name: `act_quant`: whole numbers. `gate_up_quant`: whole numbers. `down_quant`: whole numbers.
All inputs are finite; a program needn't handle non-finite values.
Results may differ from the reference program's by a relative error of at most 0.005.
Values may be sent and summed in bfloat16 or wider, within the bound.
A program may use at most 128 MiB of HBM per device.

```python
import math
import jax
import jax.numpy as jnp

D = 8192
FF = 29568
TOK = 512


def integer_levels(key, shape_dims):
    levels = jax.random.randint(key, shape_dims, -127, 128)
    return levels.astype(jnp.float32).astype(jnp.bfloat16)


def draw_act_quant(key, part):
    return integer_levels(jax.random.fold_in(key, 11), (TOK, D))


def draw_gate_up_quant(key, part):
    return integer_levels(jax.random.fold_in(key, 22), (2, D, FF))


def draw_down_quant(key, part):
    return integer_levels(jax.random.fold_in(key, 33), (FF, D))


def steps_of(rng, shape, pieces, least, top_value):
    level = 1.0
    for axis_at, parts in pieces:
        heights = jax.random.uniform(jax.random.fold_in(jax.random.fold_in(rng, 6), axis_at), (parts,), jnp.float32, least / len(pieces), top_value / len(pieces))
        level = level * jnp.repeat(jnp.exp(heights), shape[axis_at] // parts).reshape((-1,) + (1,) * (len(shape) - 1 - axis_at))
    return level


def setup_inputs(seed: int = 0) -> dict:
    keys = jax.random.split(jax.random.key(seed), 7)
    return {
        "act_quant": draw_act_quant(jax.random.fold_in(keys[6], 71), 0),
        "act_scale": jnp.clip(jnp.exp(jax.random.uniform(keys[1], (TOK,), jnp.float32, math.log(0.004), math.log(0.04))), 0.004, 0.04),
        "gate_up_quant": draw_gate_up_quant(jax.random.fold_in(keys[6], 71), 0),
        "gate_up_scale": jnp.clip(jnp.exp(math.log(0.0005) - 2.3025852 * jax.random.uniform(keys[3], (2, FF), jnp.float32) ** steps_of(keys[3], (2, FF), ((1, 8),), -0.2, 0.2)), 4.999999873689376e-05, 0.0005),
        "down_quant": draw_down_quant(jax.random.fold_in(keys[6], 71), 0),
        "down_scale": jnp.clip(jnp.exp(math.log(0.0003) - 2.3025852 * jax.random.uniform(keys[5], (D,), jnp.float32) ** steps_of(keys[5], (D,), ((0, 4),), -0.2, 0.2)), 2.9999999242136255e-05, 0.0003),
    }


def reference(act_quant, act_scale, gate_up_quant, gate_up_scale, down_quant, down_scale):
    gate_acc = jnp.dot(act_quant, gate_up_quant[0], preferred_element_type=jnp.float32)
    up_acc = jnp.dot(act_quant, gate_up_quant[1], preferred_element_type=jnp.float32)
    gate_val = gate_acc * act_scale[:, None] * gate_up_scale[0][None, :]
    up_val = up_acc * act_scale[:, None] * gate_up_scale[1][None, :]
    hidden = (jax.nn.silu(gate_val) * up_val).astype(jnp.bfloat16)
    out_acc = jnp.dot(hidden, down_quant, preferred_element_type=jnp.float32)
    return (out_acc * down_scale[None, :]).astype(jnp.bfloat16)
```

```python
import functools

import jax
import jax.numpy as jnp
from jax import lax
from jax.experimental import pallas as pl
from jax.experimental.pallas import tpu as pltpu
from jax.sharding import PartitionSpec as P

MESH = pl.DeviceIdType.MESH
SMALL, LARGE = 8, 16
RING = 3
FIRST = (512, 1024)
GTILE = 1280
DTILE = 1024
VTILE = 512
TTILE = 512
F32, BF16 = jnp.float32, jnp.bfloat16
sc = jax.named_scope


def pieces(width, size):
    return [(s, min(size, width - s)) for s in range(0, width, size)]


def blocks_of(width):
    out, start = [], 0
    for size in FIRST:
        if start + size < width:
            out.append((start, size))
            start += size
    return out + [(start + s, w) for s, w in pieces(width - start, GTILE)]


def chunks_of(tokens):
    if tokens % LARGE or tokens < 2 * LARGE:
        return [SMALL] * (tokens // SMALL)
    return [LARGE] * (tokens // LARGE - 1) + [SMALL] * 2


def hop(v, d, n):
    if n & (n - 1):
        return lax.rem(v + d, n)
    r, bit = 0, 1
    while bit < n:
        b = lax.rem(v // bit, 2)
        r = r + bit * ((1 - b) if d & bit else b)
        bit *= 2
    return r


def back(v, d, n):
    return lax.rem(v + n - d, n) if n & (n - 1) else hop(v, d, n)


def for_tiles(start, width, fn, size=VTILE):
    full = width // size
    if full:
        def step(j, carry):
            fn(pl.ds(pl.multiple_of(start + j * size, 128), size))
            return carry
        lax.fori_loop(0, full, step, 0)
    if width % size:
        fn(pl.ds(start + full * size, width % size))


def kernel(ns, Rz, Ry, X, act, act_scale, gu_hbm, gu_scale, down_hbm, down_scale, out, *scratch):
    K = len(ns)
    it_ = iter(scratch)
    take = lambda: next(it_)
    wt, wdn, keep, dsend, drecv, xsend, opart, ysend, zsend, packed = (take() for _ in range(10))
    acts = [take() for _ in ns]
    xrecv = [take() for _ in range(RING)]
    hid = [take() for _ in range(RING)]
    yrecv = [take() for _ in ns]
    zrecv = [take() for _ in ns]
    zown = [take() for _ in ns]
    (w_sem, az_s, az_r, ay_s, ay_r, d_s, d_r, x_s, x_r, h_s, h_r, p_s, p_r, f_s, f_r,
     y_s, y_r, z_s, z_r, credit) = (take() for _ in range(20))

    R, C = Rz * Ry, X * 2
    _, Dl, Fl = wt.shape
    tpr = act.shape[0]
    tok = act_scale.shape[1]
    offs = [sum(ns[:k]) for k in range(K)]
    fblk = blocks_of(Fl)
    NB = len(fblk)
    dblk = pieces(Dl, DTILE)
    nb = R // C
    row, col = lax.axis_index("row"), lax.axis_index("col")
    z, y = row // Ry, lax.rem(row, Ry)
    x, core = col // 2, lax.rem(col, 2)
    pos = core * X + x
    partner = {"row": row, "col": x * 2 + 1 - core}

    def zdev(d):
        return {"row": hop(z, d, Rz) * Ry + y, "col": col}

    def ydev(d):
        return {"row": z * Ry + hop(y, d, Ry), "col": col}

    def xdev(d):
        return {"row": row, "col": hop(x, d, X) * 2 + core}

    def remote(src, dst, s, r, dev):
        return pltpu.make_async_remote_copy(src_ref=src, dst_ref=dst, send_sem=s, recv_sem=r,
                                            device_id=dev, device_id_type=MESH)

    nfull = Fl // TTILE
    tail = Fl - nfull * TTILE

    def wrows(i, size=TTILE):
        return pl.ds(pl.multiple_of(i * TTILE, TTILE) if not isinstance(i, int) else i * TTILE, size)

    def wcopy(g, i, size=TTILE):
        src = gu_hbm.at[g] if g < 2 else down_hbm
        return pltpu.make_async_copy(src.at[wrows(i, size)], wdn.at[wrows(i, size)], w_sem.at[i])

    for i in range(nfull):
        wcopy(0, i).start()
    if tail:
        wcopy(0, nfull, tail).start()

    barrier = pltpu.get_barrier_semaphore()
    peers = ([zdev(d) for d in range(1, Rz)] + [ydev(d) for d in range(1, Ry)]
             + [xdev(d) for d in range(1, X)] + [partner])
    for p in peers:
        pl.semaphore_signal(barrier, inc=1, device_id=p, device_id_type=MESH)

    def turn(g, i, size):
        wcopy(g, i, size).wait()
        half = Dl // 2
        cols = wrows(i, size)

        def part(c, carry):
            rows = pl.ds(pl.multiple_of(c * half, half), half)
            wt[g, rows, cols] = wdn[wrows(i, size), rows].T
            return carry
        lax.fori_loop(0, 2, part, 0)
        wcopy(g + 1, i, size).start()

    def turns(g, lo, hi):
        def step(i, carry):
            turn(g, i, TTILE)
            return carry
        with sc(f"T{g}_{lo}"):
            if hi > lo:
                lax.fori_loop(lo, min(hi, nfull), step, 0)
            if hi > nfull and tail:
                turn(g, nfull, tail)

    with sc("barrier"):
        pl.semaphore_wait(barrier, len(peers))

    az = [[remote(act.at[pl.ds(offs[k], n)], acts[k].at[y, z], az_s.at[k, d - 1], az_r.at[k, d - 1], zdev(d))
           for d in range(1, Rz)] for k, n in enumerate(ns)]
    ay = [[[remote(act.at[pl.ds(offs[k], n)] if d == 0 else acts[k].at[y, back(z, d, Rz)],
                   acts[k].at[y, z if d == 0 else back(z, d, Rz)],
                   ay_s.at[k, d, e - 1], ay_r.at[k, d, e - 1], ydev(e))
            for e in range(1, Ry)] for d in range(Rz)] for k, n in enumerate(ns)]

    def gather(k):
        for c in az[k]:
            c.start()
        for c in ay[k][0]:
            c.start()
        acts[k][y, z] = act[offs[k]:offs[k] + ns[k], :]

    def forward(k, d):
        with sc(f"w_az{k}_{d}"):
            az[k][d - 1].wait_recv()
        for c in ay[k][d]:
            c.start()

    gather(0)

    T = [R * n for n in ns]
    own = [t // C for t in T]
    cols_of = [pl.ds(s, w) for s, w in fblk]
    dd = [[remote(dsend.at[:, pl.ds(0, T[k] // 2), c], drecv.at[:, pl.ds(0, T[k] // 2), c],
                  d_s.at[b], d_r.at[b], partner) for b, c in enumerate(cols_of)] for k in range(K)]
    xx = [[[remote(xsend.at[k % 2, d - 1, :, pl.ds(0, own[k]), c], xrecv[k % RING].at[d - 1, :, pl.ds(0, own[k]), c],
                   x_s.at[k % 2, b, d - 1], x_r.at[k % RING, b, d - 1], xdev(d)) for d in range(1, X)]
           for b, c in enumerate(cols_of)] for k in range(K)]
    hh = [[[remote(hid[k % RING].at[pos, pl.ds(0, own[k]), c], hid[k % RING].at[pos, pl.ds(0, own[k]), c],
                   h_s.at[k % RING, b, d - 1], h_r.at[k % RING, b, d - 1], xdev(d)) for d in range(1, X)]
           for b, c in enumerate(cols_of)] for k in range(K)]
    hp = [[remote(hid[k % RING].at[pos, pl.ds(0, own[k]), c], hid[k % RING].at[pos, pl.ds(0, own[k]), c], p_s.at[k % RING, b], p_r.at[k % RING, b], partner)
           for b, c in enumerate(cols_of)] for k in range(K)]
    ff = [[[remote(hid[k % RING].at[core * X + back(x, d, X), pl.ds(0, own[k]), c], hid[k % RING].at[core * X + back(x, d, X), pl.ds(0, own[k]), c],
                   f_s.at[k % 2, b, d - 1], f_r.at[k % RING, b, d - 1], partner) for d in range(1, X)]
           for b, c in enumerate(cols_of)] for k in range(K)]
    yy = [[[remote(ysend.at[k % 2, d - 1, :, pl.ds(0, ns[k]), pl.ds(s, w)], yrecv[k].at[d - 1, :, :, pl.ds(s, w)],
                   y_s.at[k % 2, t, d - 1], y_r.at[k, t, d - 1], ydev(d)) for d in range(1, Ry)]
           for t, (s, w) in enumerate(dblk)] for k in range(K)]
    zz = [[[remote(zsend.at[k % 2, d - 1, pl.ds(0, ns[k]), pl.ds(s, w)], zrecv[k].at[d - 1, :, pl.ds(s, w)],
                   z_s.at[k % 2, t, d - 1], z_r.at[k, t, d - 1], zdev(d)) for d in range(1, Rz)]
           for t, (s, w) in enumerate(dblk)] for k in range(K)]

    def stage_g(k, b):
        if b == 0:
            with sc(f"w_ay{k}"):
                for d in range(Rz):
                    for c in ay[k][d]:
                        c.wait_recv()
        if k >= 1:
            dd[k - 1][b].wait_send()
        hy, half = Ry // 2, T[k] // 2
        cols = cols_of[b]
        repack = ns[k] < LARGE

        def operand():
            return jnp.concatenate([acts[k][pl.ds(core * hy, hy)].reshape(half, Dl),
                                    acts[k][pl.ds((1 - core) * hy, hy)].reshape(half, Dl)], axis=0)
        if repack and b == 0:
            with sc(f"pack{k}"):
                packed[...] = operand()

        def one(g, carry):
            lhs = jnp.concatenate([packed[...]] * 2, axis=0) if repack else operand()
            r = jnp.dot(lhs, wt[g, :, cols], preferred_element_type=F32)
            keep[k % 2, g, pl.ds(0, half), cols] = r[:half]
            dsend[g, pl.ds(0, half), cols] = r[half:T[k]]
            return carry
        with sc(f"G{k}_{b}"):
            lax.fori_loop(0, 2, one, 0)
        if k >= 1:
            pl.semaphore_wait(credit, 1)
        dd[k][b].start()

    def stage_x(k, b):
        with sc(f"w_dd{k}_{b}"):
            dd[k][b].wait_recv()
        if k >= 2:
            for c in xx[k - 2][b]:
                c.wait_send()
        o = own[k]
        for d in range(1, X):
            rows = pl.ds(pl.multiple_of(hop(x, d, X) * o, o), o)
            for g in range(2):
                def tile(cols, g=g, rows=rows, d=d):
                    xsend[k % 2, d - 1, g, pl.ds(0, o), cols] = (
                        keep[k % 2, g, rows, cols] + drecv[g, rows, cols]).astype(BF16)
                for_tiles(*fblk[b], tile)
            xx[k][b][d - 1].start()
        rows = pl.ds(pl.multiple_of(x * o, o), o)
        for g in range(2):
            def tile(cols, g=g):
                keep[k % 2, g, rows, cols] = keep[k % 2, g, rows, cols] + drecv[g, rows, cols]
            for_tiles(*fblk[b], tile)
        if k + 1 < K:
            pl.semaphore_signal(credit, inc=1, device_id=partner, device_id_type=MESH)

    def stage_s(k):
        o, n = own[k], ns[k]
        scales = []
        for i in range(nb):
            blk = pos * nb + i
            first = (lax.rem(blk, Rz) * Ry + blk // Rz) * tpr + offs[k]
            want = first + lax.broadcasted_iota(jnp.int32, (n, tok), 0)
            hit = lax.broadcasted_iota(jnp.int32, (n, tok), 1) == want
            scales.append(jnp.sum(jnp.where(hit, act_scale[...], 0.0), axis=1, keepdims=True))
        scale = jnp.concatenate(scales, axis=0)
        rows = pl.ds(pl.multiple_of(x * o, o), o)
        for b in range(NB):
            with sc(f"w_xx{k}_{b}"):
                for c in xx[k][b]:
                    c.wait_recv()

            def tile(cols):
                vals = []
                for g in range(2):
                    v = keep[k % 2, g, rows, cols]
                    for d in range(1, X):
                        v = v + xrecv[k % RING][d - 1, g, pl.ds(0, o), cols].astype(F32)
                    vals.append(v * scale * gu_scale[g:g + 1, cols])
                hid[k % RING][pos, pl.ds(0, o), cols] = (vals[0] / (1.0 + jnp.exp(-vals[0])) * vals[1]).astype(BF16)
            with sc(f"S{k}_{b}"):
                for_tiles(*fblk[b], tile)
            for c in hh[k][b]:
                c.start()
            hp[k][b].start()

    def stage_h(k):
        for b in range(NB):
            with sc(f"w_hh{k}_{b}"):
                for c in hh[k][b]:
                    c.wait_recv()
            for c in ff[k][b]:
                c.start()

    def ready_d(k):
        if k == 0:
            with sc("w_down"):
                for i in range(nfull):
                    wcopy(2, i).wait()
                if tail:
                    wcopy(2, nfull, tail).wait()
        if k >= 2:
            for t in range(len(dblk)):
                for c in yy[k - 2][t]:
                    c.wait_send()
        with sc(f"w_ff{k}"):
            for b in range(NB):
                hp[k][b].wait_recv()
                for c in ff[k][b]:
                    c.wait_recv()

    def after_d(k):
        for c in sum(ff[k], []):
            c.wait_send()

    def stage_d(k):
        ready_d(k)
        for t in range(len(dblk)):
            down_tile(k, t)
        after_d(k)

    def down_tile(k, t):
        n, per = ns[k], C // Ry
        s, w = dblk[t]
        with sc(f"D{k}_{t}"):
            lhs = [hid[k % RING][pl.ds(hop(y, d, Ry) * per, per), pl.ds(0, own[k])].reshape(T[k] // Ry, Fl)
                   for d in range(Ry)]
            lhs = jnp.concatenate(lhs * (LARGE // n), axis=0)
            r = jnp.dot(lhs, wdn[:, pl.ds(s, w)], preferred_element_type=F32)[:T[k]].reshape(Ry, Rz, n, w)
            opart[k % 2, :, pl.ds(0, n), pl.ds(s, w)] = r[0]
            for d in range(1, Ry):
                ysend[k % 2, d - 1, :, pl.ds(0, n), pl.ds(s, w)] = r[d].astype(BF16)
        for c in yy[k][t]:
            c.start()

    def stage_y(k, only=None):
        n = ns[k]
        for t, (s, w) in enumerate(dblk):
            if only is not None and t not in only:
                continue
            with sc(f"w_yy{k}_{t}"):
                for c in yy[k][t]:
                    c.wait_recv()
            if k >= 2:
                for c in zz[k - 2][t]:
                    c.wait_send()
            cols = pl.ds(s, w)
            for d in range(1, Rz + 1):
                zt = hop(z, d, Rz) if d < Rz else z
                v = opart[k % 2, zt, pl.ds(0, n), cols]
                for e in range(1, Ry):
                    v = v + yrecv[k][e - 1, zt, :, cols].astype(F32)
                if d < Rz:
                    zsend[k % 2, d - 1, pl.ds(0, n), cols] = v.astype(BF16)
                    zz[k][t][d - 1].start()
                else:
                    zown[k][:, cols] = v

    def stage_z(k):
        for t, (s, w) in enumerate(dblk):
            with sc(f"w_zz{k}_{t}"):
                for c in zz[k][t]:
                    c.wait_recv()
            cols = pl.ds(s, w)
            v = zown[k][:, cols]
            for d in range(1, Rz):
                v = v + zrecv[k][d - 1, :, cols].astype(F32)
            out[offs[k]:offs[k] + ns[k], cols] = (v * down_scale[:, cols]).astype(BF16)

    order = [(0, i) for i in range(nfull + 1)] + [(1, i) for i in range(nfull + 1)]
    stops = [min((nfull + 1) * (d + 1) // 2, len(order)) for d in range(Rz - 1)] + [len(order)]
    done = 0
    for d, stop in enumerate(stops):
        for g in range(2):
            mine = [i for h, i in order[done:stop] if h == g]
            if mine:
                turns(g, mine[0], mine[-1] + 1)
        done = stop
        if d < Rz - 1:
            forward(0, d + 1)
            if d == min(1, Rz - 2) and K > 1:
                gather(1)

    def settle(k):
        for c in az[k] + sum(ay[k], []) + sum(hh[k], []) + hp[k]:
            c.wait_send()

    last = len(dblk) - 1
    for it in range(K):
        late = it == K - 2 and it >= 2
        for b in range(NB):
            stage_g(it, b)
            if b >= 1 and not late:
                stage_x(it, b - 1)
            if it + 1 < K:
                for d in range(1, Rz):
                    if min(d - 1, NB - 1) == b:
                        forward(it + 1, d)
            if b == min(2, NB - 1) and it + 2 < K:
                gather(it + 2)
        if late:
            stage_s(it - 1)
        for b in range(0 if late else NB - 1, NB):
            stage_x(it, b)
        if it >= 3:
            stage_y(it - 3)
        if it >= 2 and it == K - 1:
            stage_h(it - 2)
            stage_d(it - 2)
        if it >= 1 and not late:
            stage_s(it - 1)
        if it >= 2 and it < K - 1:
            stage_h(it - 2)
            stage_d(it - 2)
        if it >= 3:
            settle(it - 3)
        if it >= 4:
            stage_z(it - 4)
    if K >= 3:
        settle(K - 3)
    if K >= 2:
        for c in sum(xx[K - 2], []):
            c.wait_send()
    stage_s(K - 1)
    if K >= 3:
        stage_y(K - 3, range(last))
    if K >= 2:
        stage_h(K - 2)
    if K >= 3:
        stage_y(K - 3, (last,))
    if K >= 2:
        ready_d(K - 2)
    for t in range(len(dblk)):
        if K >= 2:
            down_tile(K - 2, t)
        if t == 0:
            stage_h(K - 1)
    ready_d(K - 1)
    for t in range(len(dblk)):
        down_tile(K - 1, t)
        if K >= 2:
            stage_y(K - 2, (t,))
    for k in range(max(K - 2, 0), K):
        after_d(k)
        settle(k)
    for c in dd[K - 1] + sum(xx[K - 1], []):
        c.wait_send()
    if K >= 4:
        stage_z(K - 4)
    stage_y(K - 1)
    for k in range(max(K - 2, 0), K):
        for c in sum(yy[k], []):
            c.wait_send()
    for k in range(max(K - 3, 0), K):
        stage_z(k)
    with sc("end"):
        for k in range(max(K - 2, 0), K):
            for c in sum(zz[k], []):
                c.wait_send()


def solution(mesh):
    R, C = mesh.shape["row"], mesh.shape["col"]
    X = C // 2
    Ry = max(d for d in range(1, R + 1) if R % d == 0 and d * d <= R)
    Rz = R // Ry

    def body(act, act_scale, gu, gu_scale, down, down_scale):
        tpr, Dl = act.shape
        Fl = gu.shape[2]
        ns = chunks_of(tpr)
        K, n = len(ns), max(ns)
        T = R * n
        own = T // C
        NB, ND, NT = len(blocks_of(Fl)), len(pieces(Dl, DTILE)), len(pieces(Fl, TTILE))
        vmem = pl.BlockSpec(memory_space=pltpu.VMEM)
        hbm = pl.BlockSpec(memory_space=pl.ANY)
        dma = pltpu.SemaphoreType.DMA
        scratch = [
            pltpu.VMEM((2, Dl, Fl), BF16),
            pltpu.VMEM((Fl, Dl), BF16),
            pltpu.VMEM((2, 2, T // 2, Fl), F32),
            pltpu.VMEM((2, T // 2, Fl), F32),
            pltpu.VMEM((2, T // 2, Fl), F32),
            pltpu.VMEM((2, X - 1, 2, own, Fl), BF16),
            pltpu.VMEM((2, Rz, n, Dl), F32),
            pltpu.VMEM((2, Ry - 1, Rz, n, Dl), BF16),
            pltpu.VMEM((2, Rz - 1, n, Dl), BF16),
            pltpu.VMEM((R * SMALL, Dl), BF16),
            *[pltpu.VMEM((Ry, Rz, m, Dl), BF16) for m in ns],
            *[pltpu.VMEM((X - 1, 2, own, Fl), BF16)] * RING,
            *[pltpu.VMEM((C, own, Fl), BF16)] * RING,
            *[pltpu.VMEM((Ry - 1, Rz, m, Dl), BF16) for m in ns],
            *[pltpu.VMEM((Rz - 1, m, Dl), BF16) for m in ns],
            *[pltpu.VMEM((m, Dl), F32) for m in ns],
            dma((NT,)),
            dma((K, Rz - 1)), dma((K, Rz - 1)),
            dma((K, Rz, Ry - 1)), dma((K, Rz, Ry - 1)),
            dma((NB,)), dma((NB,)),
            dma((2, NB, X - 1)), dma((RING, NB, X - 1)),
            dma((RING, NB, X - 1)), dma((RING, NB, X - 1)),
            dma((RING, NB)), dma((RING, NB)),
            dma((2, NB, X - 1)), dma((RING, NB, X - 1)),
            dma((2, ND, Ry - 1)), dma((K, ND, Ry - 1)),
            dma((2, ND, Rz - 1)), dma((K, ND, Rz - 1)),
            pltpu.SemaphoreType.REGULAR,
        ]
        return pl.pallas_call(
            functools.partial(kernel, ns, Rz, Ry, X),
            out_shape=jax.ShapeDtypeStruct((tpr, Dl), BF16),
            in_specs=[vmem, vmem, hbm, vmem, hbm, vmem],
            out_specs=vmem,
            scratch_shapes=scratch,
            compiler_params=pltpu.CompilerParams(
                collective_id=0, has_side_effects=True, vmem_limit_bytes=67043328
            ),
        )(act, act_scale.reshape(1, -1), jnp.swapaxes(gu, 1, 2), gu_scale, down, down_scale.reshape(1, Dl))

    in_specs = (P("row", "col"), P(), P(None, "col", "row"), P(None, "row"), P("row", "col"), P("col"))
    return jax.shard_map(body, mesh=mesh, in_specs=in_specs, out_specs=P("row", "col"), check_vma=False)
```

```python
import functools

import jax
import jax.numpy as jnp
from jax import lax
from jax.experimental import pallas as pl
from jax.experimental.pallas import tpu as pltpu
from jax.sharding import PartitionSpec as P

MESH = pl.DeviceIdType.MESH
SMALL, LARGE = 8, 16
RING = 3
FIRST = (512, 1024)
GTILE = 1280
VTILE = 512
TTILE = 512
F32, BF16 = jnp.float32, jnp.bfloat16
sc = jax.named_scope


def pieces(width, size):
    return [(s, min(size, width - s)) for s in range(0, width, size)]


def tiles_of(width):
    return [(0, width // 2), (width // 2, width // 4), (width // 4 * 3, width // 4)]


def blocks_of(width):
    out, start = [], 0
    for size in FIRST:
        if start + size < width:
            out.append((start, size))
            start += size
    return out + [(start + s, w) for s, w in pieces(width - start, GTILE)]


def chunks_of(tokens):
    if tokens % LARGE or tokens < 2 * LARGE:
        return [SMALL] * (tokens // SMALL)
    return [LARGE] * (tokens // LARGE - 1) + [SMALL] * 2


def hop(v, d, n):
    if n & (n - 1):
        return lax.rem(v + d, n)
    r, bit = 0, 1
    while bit < n:
        b = lax.rem(v // bit, 2)
        r = r + bit * ((1 - b) if d & bit else b)
        bit *= 2
    return r


def back(v, d, n):
    return lax.rem(v + n - d, n) if n & (n - 1) else hop(v, d, n)


def for_tiles(start, width, fn, size=VTILE):
    full = width // size
    if full:
        def step(j, carry):
            fn(pl.ds(pl.multiple_of(start + j * size, 128), size))
            return carry
        lax.fori_loop(0, full, step, 0)
    if width % size:
        fn(pl.ds(start + full * size, width % size))


def kernel(ns, Rz, Ry, X, act_in, act_scale_in, gu_hbm, gu_scale_in, down_hbm, down_scale_in, out, *scratch):
    K = len(ns)
    it_ = iter(scratch)
    take = lambda: next(it_)
    wt, wdn, keep, dsend, drecv, xsend, opart, ysend, zsend, packed = (take() for _ in range(10))
    act, act_scale, gu_scale, down_scale, i_sem = (take() for _ in range(5))
    acts = [take() for _ in ns]
    xrecv = [take() for _ in range(RING)]
    hid = [take() for _ in range(RING)]
    yrecv = [take() for _ in ns]
    zrecv = [take() for _ in ns]
    zown = [take() for _ in ns]
    (w_sem, az_s, az_r, ay_s, ay_r, d_s, d_r, x_s, x_r, h_s, h_r, p_s, p_r, f_s,
     y_s, y_r, z_s, z_r, credit) = (take() for _ in range(19))

    R, C = Rz * Ry, X * 2
    _, Dl, Fl = wt.shape
    tpr = act.shape[0]
    tok = act_scale.shape[1]
    offs = [sum(ns[:k]) for k in range(K)]
    fblk = blocks_of(Fl)
    NB = len(fblk)
    dblk = tiles_of(Dl)
    nb = R // C
    row, col = lax.axis_index("row"), lax.axis_index("col")
    z, y = row // Ry, lax.rem(row, Ry)
    x, core = col // 2, lax.rem(col, 2)
    pos = core * X + x
    partner = {"row": row, "col": x * 2 + 1 - core}

    def zdev(d):
        return {"row": hop(z, d, Rz) * Ry + y, "col": col}

    def ydev(d):
        return {"row": z * Ry + hop(y, d, Ry), "col": col}

    def xdev(d):
        return {"row": row, "col": hop(x, d, X) * 2 + core}

    def remote(src, dst, s, r, dev):
        return pltpu.make_async_remote_copy(src_ref=src, dst_ref=dst, send_sem=s, recv_sem=r,
                                            device_id=dev, device_id_type=MESH)

    nfull = Fl // TTILE
    tail = Fl - nfull * TTILE

    def wrows(i, size=TTILE):
        return pl.ds(pl.multiple_of(i * TTILE, TTILE) if not isinstance(i, int) else i * TTILE, size)

    def wcopy(g, i, size=TTILE):
        src = gu_hbm.at[g] if g < 2 else down_hbm
        return pltpu.make_async_copy(src.at[wrows(i, size)], wdn.at[wrows(i, size)], w_sem.at[i])

    inputs = [pltpu.make_async_copy(a, b, i_sem.at[i]) for i, (a, b) in enumerate(
        ((act_in, act), (act_scale_in, act_scale), (gu_scale_in, gu_scale), (down_scale_in, down_scale)))]
    inputs[0].start()
    barrier = pltpu.get_barrier_semaphore()
    peers = ([zdev(d) for d in range(1, Rz)] + [ydev(d) for d in range(1, Ry)]
             + [xdev(d) for d in range(1, X)] + [partner])
    for p in peers:
        pl.semaphore_signal(barrier, inc=1, device_id=p, device_id_type=MESH)

    def turn(g, i, size):
        wcopy(g, i, size).wait()
        half = Dl // 2
        cols = wrows(i, size)

        def part(c, carry):
            rows = pl.ds(pl.multiple_of(c * half, half), half)
            wt[g, rows, cols] = wdn[wrows(i, size), rows].T
            return carry
        lax.fori_loop(0, 2, part, 0)
        wcopy(g + 1, i, size).start()

    def turns(g, lo, hi):
        def step(i, carry):
            turn(g, i, TTILE)
            return carry
        with sc(f"T{g}_{lo}"):
            if hi > lo:
                lax.fori_loop(lo, min(hi, nfull), step, 0)
            if hi > nfull and tail:
                turn(g, nfull, tail)

    with sc("w_act"):
        inputs[0].wait()
    for i in range(nfull):
        wcopy(0, i).start()
    if tail:
        wcopy(0, nfull, tail).start()
    for c in inputs[1:]:
        c.start()
    with sc("barrier"):
        pl.semaphore_wait(barrier, len(peers))

    az = [[remote(act.at[pl.ds(offs[k], n)], acts[k].at[y, z], az_s.at[k, d - 1], az_r.at[k, d - 1], zdev(d))
           for d in range(1, Rz)] for k, n in enumerate(ns)]
    ay = [[[remote(act.at[pl.ds(offs[k], n)] if d == 0 else acts[k].at[y, back(z, d, Rz)],
                   acts[k].at[y, z if d == 0 else back(z, d, Rz)],
                   ay_s.at[k, d, e - 1], ay_r.at[k, e - 1], ydev(e))
            for e in range(1, Ry)] for d in range(Rz)] for k, n in enumerate(ns)]

    ay_all = [[remote(acts[k].at[hop(y, e, Ry)], acts[k].at[hop(y, e, Ry)],
                      ay_s.at[k, 0, e - 1], ay_r.at[k, e - 1], ydev(e)) for e in range(1, Ry)] for k in range(K)]

    def gather(k):
        for c in az[k]:
            c.start()
        for c in ay[k][0]:
            c.start()
        acts[k][y, z] = act[offs[k]:offs[k] + ns[k], :]

    def forward(k, d):
        with sc(f"w_az{k}_{d}"):
            az[k][d - 1].wait_recv()
        for c in ay[k][d]:
            c.start()

    gather(0)

    T = [R * n for n in ns]
    own = [t // C for t in T]
    cols_of = [pl.ds(s, w) for s, w in fblk]
    dd = [[remote(dsend.at[:, pl.ds(0, T[k] // 2), c], drecv.at[:, pl.ds(0, T[k] // 2), c],
                  d_s.at[b], d_r.at[b], partner) for b, c in enumerate(cols_of)] for k in range(K)]
    xx = [[[remote(xsend.at[k % 2, d - 1, :, pl.ds(0, own[k]), c], xrecv[k % RING].at[d - 1, :, pl.ds(0, own[k]), c],
                   x_s.at[k % 2, b, d - 1], x_r.at[k % RING, b, d - 1], xdev(d)) for d in range(1, X)]
           for b, c in enumerate(cols_of)] for k in range(K)]
    hh = [[[remote(hid[k % RING].at[pos, pl.ds(0, own[k]), c], hid[k % RING].at[pos, pl.ds(0, own[k]), c],
                   h_s.at[k % RING, b, d - 1], h_r.at[k % RING, b, d - 1], xdev(d)) for d in range(1, X)]
           for b, c in enumerate(cols_of)] for k in range(K)]
    hp = [[remote(hid[k % RING].at[pos, pl.ds(0, own[k]), c], hid[k % RING].at[pos, pl.ds(0, own[k]), c], p_s.at[k % RING, b], p_r.at[k % RING], partner)
           for b, c in enumerate(cols_of)] for k in range(K)]
    ff = [[[remote(hid[k % RING].at[core * X + back(x, d, X), pl.ds(0, own[k]), c], hid[k % RING].at[core * X + back(x, d, X), pl.ds(0, own[k]), c],
                   f_s.at[k % 2, b, d - 1], p_r.at[k % RING], partner) for d in range(1, X)]
           for b, c in enumerate(cols_of)] for k in range(K)]
    yy = [[[remote(ysend.at[k % 2, d - 1, :, pl.ds(0, ns[k]), pl.ds(s, w)], yrecv[k].at[d - 1, :, :, pl.ds(s, w)],
                   y_s.at[k % 2, t, d - 1], y_r.at[k, t, d - 1], ydev(d)) for d in range(1, Ry)]
           for t, (s, w) in enumerate(dblk)] for k in range(K)]
    zz = [[[remote(zsend.at[k % 2, d - 1, pl.ds(0, ns[k]), pl.ds(s, w)], zrecv[k].at[d - 1, :, pl.ds(s, w)],
                   z_s.at[k % 2, t, d - 1], z_r.at[k, t], zdev(d)) for d in range(1, Rz)]
           for t, (s, w) in enumerate(dblk)] for k in range(K)]

    def stage_g(k, b):
        if b == 0:
            with sc(f"w_ay{k}"):
                for c in ay_all[k]:
                    c.wait_recv()
        if k >= 1:
            dd[k - 1][b].wait_send()
        hy, half = Ry // 2, T[k] // 2
        cols = cols_of[b]
        repack = ns[k] < LARGE

        def operand():
            return jnp.concatenate([acts[k][pl.ds(core * hy, hy)].reshape(half, Dl),
                                    acts[k][pl.ds((1 - core) * hy, hy)].reshape(half, Dl)], axis=0)
        if repack and b == 0:
            with sc(f"pack{k}"):
                packed[...] = operand()

        def one(g, carry):
            lhs = jnp.concatenate([packed[...]] * 2, axis=0) if repack else operand()
            r = jnp.dot(lhs, wt[g, :, cols], preferred_element_type=F32)
            keep[k % 2, g, pl.ds(0, half), cols] = r[:half]
            dsend[g, pl.ds(0, half), cols] = r[half:T[k]]
            return carry
        with sc(f"G{k}_{b}"):
            lax.fori_loop(0, 2, one, 0)
        if k >= 1:
            pl.semaphore_wait(credit, 1)
        dd[k][b].start()

    def stage_x(k, b):
        with sc(f"w_dd{k}_{b}"):
            dd[k][b].wait_recv()
        if k >= 2:
            for c in xx[k - 2][b]:
                c.wait_send()
        o = own[k]
        for d in range(1, X):
            rows = pl.ds(pl.multiple_of(hop(x, d, X) * o, o), o)
            for g in range(2):
                def tile(cols, g=g, rows=rows, d=d):
                    xsend[k % 2, d - 1, g, pl.ds(0, o), cols] = (
                        keep[k % 2, g, rows, cols] + drecv[g, rows, cols]).astype(BF16)
                for_tiles(*fblk[b], tile)
            xx[k][b][d - 1].start()
        rows = pl.ds(pl.multiple_of(x * o, o), o)
        for g in range(2):
            def tile(cols, g=g):
                keep[k % 2, g, rows, cols] = keep[k % 2, g, rows, cols] + drecv[g, rows, cols]
            for_tiles(*fblk[b], tile)
        if k + 1 < K:
            pl.semaphore_signal(credit, inc=1, device_id=partner, device_id_type=MESH)

    def stage_s(k):
        o, n = own[k], ns[k]
        scales = []
        for i in range(nb):
            blk = pos * nb + i
            first = (lax.rem(blk, Rz) * Ry + blk // Rz) * tpr + offs[k]
            want = first + lax.broadcasted_iota(jnp.int32, (n, tok), 0)
            hit = lax.broadcasted_iota(jnp.int32, (n, tok), 1) == want
            scales.append(jnp.sum(jnp.where(hit, act_scale[...], 0.0), axis=1, keepdims=True))
        scale = jnp.concatenate(scales, axis=0)
        rows = pl.ds(pl.multiple_of(x * o, o), o)
        for b in range(NB):
            with sc(f"w_xx{k}_{b}"):
                for c in xx[k][b]:
                    c.wait_recv()

            def tile(cols):
                vals = []
                for g in range(2):
                    v = keep[k % 2, g, rows, cols]
                    for d in range(1, X):
                        v = v + xrecv[k % RING][d - 1, g, pl.ds(0, o), cols].astype(F32)
                    vals.append(v * scale * gu_scale[g:g + 1, cols])
                hid[k % RING][pos, pl.ds(0, o), cols] = (vals[0] / (1.0 + jnp.exp(-vals[0])) * vals[1]).astype(BF16)
            with sc(f"S{k}_{b}"):
                for_tiles(*fblk[b], tile)
            for c in hh[k][b]:
                c.start()
            hp[k][b].start()

    def stage_h(k, blocks=None):
        for b in range(NB) if blocks is None else blocks:
            with sc(f"w_hh{k}_{b}"):
                for c in hh[k][b]:
                    c.wait_recv()
            for c in ff[k][b]:
                c.start()

    def ready_d(k):
        if k == 0:
            with sc("w_down"):
                for i in range(nfull):
                    wcopy(2, i).wait()
                if tail:
                    wcopy(2, nfull, tail).wait()
        if k >= 2:
            for t in range(len(dblk)):
                for c in yy[k - 2][t]:
                    c.wait_send()
        with sc(f"w_ff{k}"):
            theirs = hid[k % RING].at[pl.ds((1 - core) * X, X), pl.ds(0, own[k])]
            remote(theirs, theirs, p_s.at[k % RING, 0], p_r.at[k % RING], partner).wait_recv()

    def after_d(k):
        for c in sum(ff[k], []):
            c.wait_send()

    def stage_d(k):
        ready_d(k)
        for t in range(len(dblk)):
            down_tile(k, t)
        after_d(k)

    def down_tile(k, t):
        n, per = ns[k], C // Ry
        s, w = dblk[t]
        with sc(f"D{k}_{t}"):
            lhs = [hid[k % RING][pl.ds(hop(y, d, Ry) * per, per), pl.ds(0, own[k])].reshape(T[k] // Ry, Fl)
                   for d in range(Ry)]
            lhs = jnp.concatenate(lhs * (LARGE // n), axis=0)
            r = jnp.dot(lhs, wdn[:, pl.ds(s, w)], preferred_element_type=F32)[:T[k]].reshape(Ry, Rz, n, w)
            opart[k % 2, :, pl.ds(0, n), pl.ds(s, w)] = r[0]
            for d in range(1, Ry):
                ysend[k % 2, d - 1, :, pl.ds(0, n), pl.ds(s, w)] = r[d].astype(BF16)
        for c in yy[k][t]:
            c.start()

    def stage_y(k, only=None):
        n = ns[k]
        for t, (s, w) in enumerate(dblk):
            if only is not None and t not in only:
                continue
            with sc(f"w_yy{k}_{t}"):
                for c in yy[k][t]:
                    c.wait_recv()
            if k >= 2:
                for c in zz[k - 2][t]:
                    c.wait_send()
            cols = pl.ds(s, w)
            for d in range(1, Rz + 1):
                zt = hop(z, d, Rz) if d < Rz else z
                v = opart[k % 2, zt, pl.ds(0, n), cols]
                for e in range(1, Ry):
                    v = v + yrecv[k][e - 1, zt, :, cols].astype(F32)
                if d < Rz:
                    zsend[k % 2, d - 1, pl.ds(0, n), cols] = v.astype(BF16)
                    zz[k][t][d - 1].start()
                else:
                    zown[k][:, cols] = v

    def stage_z(k):
        for t, (s, w) in enumerate(dblk):
            with sc(f"w_zz{k}_{t}"):
                cols = pl.ds(s, w)
                remote(zrecv[k].at[:, :, cols], zrecv[k].at[:, :, cols], z_s.at[k % 2, t, 0], z_r.at[k, t],
                       zdev(1)).wait_recv()
            v = zown[k][:, cols]
            for d in range(1, Rz):
                v = v + zrecv[k][d - 1, :, cols].astype(F32)
            out[offs[k]:offs[k] + ns[k], cols] = (v * down_scale[:, cols]).astype(BF16)

    order = [(0, i) for i in range(nfull + 1)] + [(1, i) for i in range(nfull + 1)]
    stops = [min(6 + 7 * d // 2, len(order)) for d in range(Rz - 1)] + [len(order)]
    done = 0
    for d, stop in enumerate(stops):
        for g in range(2):
            mine = [i for h, i in order[done:stop] if h == g]
            if mine:
                turns(g, mine[0], mine[-1] + 1)
        done = stop
        if d < Rz - 1:
            forward(0, d + 1)
            if d == min(1, Rz - 2) and K > 1:
                gather(1)

    def settle(k):
        for c in az[k] + sum(ay[k], []) + sum(hh[k], []) + hp[k]:
            c.wait_send()

    for c in inputs[1:]:
        c.wait()
    for it in range(K):
        late = it == 3
        for b in range(NB):
            stage_g(it, b)
            if b >= 1 and not late:
                stage_x(it, b - 1)
            if it + 1 < K:
                for d in range(1, Rz):
                    if min(d - 1, NB - 1) == b:
                        forward(it + 1, d)
            if b == min(2, NB - 1) and it + 2 < K:
                gather(it + 2)
        if late:
            stage_s(it - 1)
        for b in range(0 if late else NB - 1, NB):
            stage_x(it, b)
        if it >= 3:
            stage_y(it - 3)
        if it >= 1 and not late:
            stage_s(it - 1)
        if it >= 2:
            stage_h(it - 2)
            stage_d(it - 2)
        if it >= 3:
            settle(it - 3)
        if it >= 4:
            stage_z(it - 4)
    if K >= 3:
        settle(K - 3)
    if K >= 2:
        for c in sum(xx[K - 2], []):
            c.wait_send()
    stage_s(K - 1)
    if K >= 2:
        stage_h(K - 2, range(NB - 1))
    if K >= 3:
        stage_y(K - 3, (0,))
    if K >= 2:
        stage_h(K - 2, (NB - 1,))
        ready_d(K - 2)
    for t in range(len(dblk)):
        if K >= 2:
            down_tile(K - 2, t)
        if K >= 3 and t + 1 < len(dblk):
            stage_y(K - 3, (t + 1,))
        if t == 0:
            stage_h(K - 1)
    ready_d(K - 1)
    for t in range(len(dblk)):
        down_tile(K - 1, t)
    if K >= 2:
        stage_y(K - 2)
    stage_y(K - 1)
    for c in dd[K - 1] + sum(xx[K - 1], []):
        c.wait_send()
    for k in range(max(K - 2, 0), K):
        after_d(k)
        settle(k)
    if K >= 4:
        stage_z(K - 4)
    for k in range(max(K - 2, 0), K):
        for c in sum(yy[k], []):
            c.wait_send()
    for k in range(max(K - 3, 0), K):
        stage_z(k)
    with sc("end"):
        for k in range(max(K - 2, 0), K):
            for c in sum(zz[k], []):
                c.wait_send()


def solution(mesh):
    R, C = mesh.shape["row"], mesh.shape["col"]
    X = C // 2
    Ry = max(d for d in range(1, R + 1) if R % d == 0 and d * d <= R)
    Rz = R // Ry

    def body(act, act_scale, gu, gu_scale, down, down_scale):
        tpr, Dl = act.shape
        Fl = gu.shape[2]
        ns = chunks_of(tpr)
        K, n = len(ns), max(ns)
        T = R * n
        own = T // C
        NB, ND, NT = len(blocks_of(Fl)), len(tiles_of(Dl)), len(pieces(Fl, TTILE))
        vmem = pl.BlockSpec(memory_space=pltpu.VMEM)
        hbm = pl.BlockSpec(memory_space=pl.ANY)
        dma = pltpu.SemaphoreType.DMA
        scratch = [
            pltpu.VMEM((2, Dl, Fl), BF16),
            pltpu.VMEM((Fl, Dl), BF16),
            pltpu.VMEM((2, 2, T // 2, Fl), F32),
            pltpu.VMEM((2, T // 2, Fl), F32),
            pltpu.VMEM((2, T // 2, Fl), F32),
            pltpu.VMEM((2, X - 1, 2, own, Fl), BF16),
            pltpu.VMEM((2, Rz, n, Dl), F32),
            pltpu.VMEM((2, Ry - 1, Rz, n, Dl), BF16),
            pltpu.VMEM((2, Rz - 1, n, Dl), BF16),
            pltpu.VMEM((R * SMALL, Dl), BF16),
            pltpu.VMEM(act.shape, BF16),
            pltpu.VMEM((1, act_scale.shape[0]), F32),
            pltpu.VMEM(gu_scale.shape, F32),
            pltpu.VMEM((1, Dl), F32),
            dma((4,)),
            *[pltpu.VMEM((Ry, Rz, m, Dl), BF16) for m in ns],
            *[pltpu.VMEM((X - 1, 2, own, Fl), BF16)] * RING,
            *[pltpu.VMEM((C, own, Fl), BF16)] * RING,
            *[pltpu.VMEM((Ry - 1, Rz, m, Dl), BF16) for m in ns],
            *[pltpu.VMEM((Rz - 1, m, Dl), BF16) for m in ns],
            *[pltpu.VMEM((m, Dl), F32) for m in ns],
            dma((NT,)),
            dma((K, Rz - 1)), dma((K, Rz - 1)),
            dma((K, Rz, Ry - 1)), dma((K, Ry - 1)),
            dma((NB,)), dma((NB,)),
            dma((2, NB, X - 1)), dma((RING, NB, X - 1)),
            dma((RING, NB, X - 1)), dma((RING, NB, X - 1)),
            dma((RING, NB)), dma((RING,)),
            dma((2, NB, X - 1)),
            dma((2, ND, Ry - 1)), dma((K, ND, Ry - 1)),
            dma((2, ND, Rz - 1)), dma((K, ND)),
            pltpu.SemaphoreType.REGULAR,
        ]
        return pl.pallas_call(
            functools.partial(kernel, ns, Rz, Ry, X),
            out_shape=pltpu.VMEM((tpr, Dl), BF16),
            in_specs=[hbm] * 6,
            out_specs=vmem,
            scratch_shapes=scratch,
            compiler_params=pltpu.CompilerParams(
                collective_id=0, has_side_effects=True, vmem_limit_bytes=67043328 - 2 * tpr * Dl * 2
            ),
        )(act, act_scale.reshape(1, -1), jnp.swapaxes(gu, 1, 2), gu_scale, down, down_scale.reshape(1, Dl))

    in_specs = (P("row", "col"), P(), P(None, "col", "row"), P(None, "row"), P("row", "col"), P("col"))
    return jax.shard_map(body, mesh=mesh, in_specs=in_specs, out_specs=P("row", "col"), check_vma=False)
```

```python
import functools

import jax
import jax.numpy as jnp
from jax import lax
from jax.experimental import pallas as pl
from jax.experimental.pallas import tpu as pltpu
from jax.sharding import PartitionSpec as P

MESH = pl.DeviceIdType.MESH
SMALL, LARGE = 8, 16
RING = 3
FIRST = (512, 1024)
GTILE = 1280
VTILE = 512
TTILE = 512
F32, BF16 = jnp.float32, jnp.bfloat16
sc = jax.named_scope


def pieces(width, size):
    return [(s, min(size, width - s)) for s in range(0, width, size)]


def tiles_of(width):
    return [(0, width // 2), (width // 2, width // 4), (width // 4 * 3, width // 4)]


def blocks_of(width):
    out, start = [], 0
    for size in FIRST:
        if start + size < width:
            out.append((start, size))
            start += size
    return out + [(start + s, w) for s, w in pieces(width - start, GTILE)]


def chunks_of(tokens):
    if tokens % LARGE or tokens < 2 * LARGE:
        return [SMALL] * (tokens // SMALL)
    return [LARGE] * (tokens // LARGE - 1) + [SMALL] * 2


def hop(v, d, n):
    if n & (n - 1):
        return lax.rem(v + d, n)
    r, bit = 0, 1
    while bit < n:
        b = lax.rem(v // bit, 2)
        r = r + bit * ((1 - b) if d & bit else b)
        bit *= 2
    return r


def back(v, d, n):
    return lax.rem(v + n - d, n) if n & (n - 1) else hop(v, d, n)


def for_tiles(start, width, fn, size=VTILE):
    full = width // size
    if full:
        def step(j, carry):
            fn(pl.ds(pl.multiple_of(start + j * size, 128), size))
            return carry
        lax.fori_loop(0, full, step, 0)
    if width % size:
        fn(pl.ds(start + full * size, width % size))


def kernel(ns, Rz, Ry, X, act_in, act_scale_in, gu_hbm, gu_scale_in, down_hbm, down_scale_in, out, *scratch):
    K = len(ns)
    it_ = iter(scratch)
    take = lambda: next(it_)
    wt, wdn, keep, dsend, drecv, xsend, opart, ysend, zsend, packed = (take() for _ in range(10))
    act, act_scale, gu_scale, down_scale, i_sem = (take() for _ in range(5))
    acts = [take() for _ in ns]
    xrecv = [take() for _ in range(RING)]
    hid = [take() for _ in range(RING)]
    yrecv = [take() for _ in ns]
    zrecv = [take() for _ in ns]
    zown = [take() for _ in ns]
    (w_sem, az_s, az_r, ay_s, ay_r, d_s, d_r, x_s, x_r, h_s, h_r, p_s, p_r, f_s,
     y_s, y_r, z_s, z_r, credit) = (take() for _ in range(19))

    R, C = Rz * Ry, X * 2
    _, Dl, Fl = wt.shape
    tpr = act.shape[0]
    tok = act_scale.shape[1]
    offs = [sum(ns[:k]) for k in range(K)]
    fblk = blocks_of(Fl)
    NB = len(fblk)
    dblk = tiles_of(Dl)
    nb = R // C
    row, col = lax.axis_index("row"), lax.axis_index("col")
    z, y = row // Ry, lax.rem(row, Ry)
    x, core = col // 2, lax.rem(col, 2)
    pos = core * X + x
    partner = {"row": row, "col": x * 2 + 1 - core}

    def zdev(d):
        return {"row": hop(z, d, Rz) * Ry + y, "col": col}

    def ydev(d):
        return {"row": z * Ry + hop(y, d, Ry), "col": col}

    def xdev(d):
        return {"row": row, "col": hop(x, d, X) * 2 + core}

    def remote(src, dst, s, r, dev):
        return pltpu.make_async_remote_copy(src_ref=src, dst_ref=dst, send_sem=s, recv_sem=r,
                                            device_id=dev, device_id_type=MESH)

    nfull = Fl // TTILE
    tail = Fl - nfull * TTILE

    def wrows(i, size=TTILE):
        return pl.ds(pl.multiple_of(i * TTILE, TTILE) if not isinstance(i, int) else i * TTILE, size)

    def wcopy(g, i, size=TTILE):
        src = gu_hbm.at[g] if g < 2 else down_hbm
        return pltpu.make_async_copy(src.at[wrows(i, size)], wdn.at[wrows(i, size)], w_sem.at[i])

    inputs = [pltpu.make_async_copy(a, b, i_sem.at[i]) for i, (a, b) in enumerate(
        ((act_in, act), (act_scale_in, act_scale), (gu_scale_in, gu_scale), (down_scale_in, down_scale)))]
    inputs[0].start()
    barrier = pltpu.get_barrier_semaphore()
    peers = ([zdev(d) for d in range(1, Rz)] + [ydev(d) for d in range(1, Ry)]
             + [xdev(d) for d in range(1, X)] + [partner])
    for p in peers:
        pl.semaphore_signal(barrier, inc=1, device_id=p, device_id_type=MESH)

    def turn(g, i, size):
        wcopy(g, i, size).wait()
        half = Dl // 2
        cols = wrows(i, size)

        def part(c, carry):
            rows = pl.ds(pl.multiple_of(c * half, half), half)
            wt[g, rows, cols] = wdn[wrows(i, size), rows].T
            return carry
        lax.fori_loop(0, 2, part, 0)
        wcopy(g + 1, i, size).start()

    def turns(g, lo, hi):
        def step(i, carry):
            turn(g, i, TTILE)
            return carry
        with sc(f"T{g}_{lo}"):
            if hi > lo:
                lax.fori_loop(lo, min(hi, nfull), step, 0)
            if hi > nfull and tail:
                turn(g, nfull, tail)

    with sc("w_act"):
        inputs[0].wait()
    for i in range(nfull):
        wcopy(0, i).start()
    if tail:
        wcopy(0, nfull, tail).start()
    for c in inputs[1:]:
        c.start()
    with sc("barrier"):
        pl.semaphore_wait(barrier, len(peers))

    az = [[remote(act.at[pl.ds(offs[k], n)], acts[k].at[y, z], az_s.at[k, d - 1], az_r.at[k, d - 1], zdev(d))
           for d in range(1, Rz)] for k, n in enumerate(ns)]
    ay = [[[remote(act.at[pl.ds(offs[k], n)] if d == 0 else acts[k].at[y, back(z, d, Rz)],
                   acts[k].at[y, z if d == 0 else back(z, d, Rz)],
                   ay_s.at[k, d, e - 1], ay_r.at[k, e - 1], ydev(e))
            for e in range(1, Ry)] for d in range(Rz)] for k, n in enumerate(ns)]

    ay_all = [[remote(acts[k].at[hop(y, e, Ry)], acts[k].at[hop(y, e, Ry)],
                      ay_s.at[k, 0, e - 1], ay_r.at[k, e - 1], ydev(e)) for e in range(1, Ry)] for k in range(K)]

    def gather(k):
        for c in az[k]:
            c.start()
        for c in ay[k][0]:
            c.start()
        acts[k][y, z] = act[offs[k]:offs[k] + ns[k], :]

    def forward(k, d):
        with sc(f"w_az{k}_{d}"):
            az[k][d - 1].wait_recv()
        for c in ay[k][d]:
            c.start()

    gather(0)

    T = [R * n for n in ns]
    own = [t // C for t in T]
    cols_of = [pl.ds(s, w) for s, w in fblk]
    dd = [[remote(dsend.at[:, pl.ds(0, T[k] // 2), c], drecv.at[:, pl.ds(0, T[k] // 2), c],
                  d_s.at[b], d_r.at[b], partner) for b, c in enumerate(cols_of)] for k in range(K)]
    xx = [[[remote(xsend.at[k % 2, d - 1, :, pl.ds(0, own[k]), c], xrecv[k % RING].at[d - 1, :, pl.ds(0, own[k]), c],
                   x_s.at[k % 2, b, d - 1], x_r.at[k % RING, b, d - 1], xdev(d)) for d in range(1, X)]
           for b, c in enumerate(cols_of)] for k in range(K)]
    hh = [[[remote(hid[k % RING].at[pos, pl.ds(0, own[k]), c], hid[k % RING].at[pos, pl.ds(0, own[k]), c],
                   h_s.at[k % RING, b, d - 1], h_r.at[k % RING, b, d - 1], xdev(d)) for d in range(1, X)]
           for b, c in enumerate(cols_of)] for k in range(K)]
    hp = [[remote(hid[k % RING].at[pos, pl.ds(0, own[k]), c], hid[k % RING].at[pos, pl.ds(0, own[k]), c], p_s.at[k % RING, b], p_r.at[k % RING], partner)
           for b, c in enumerate(cols_of)] for k in range(K)]
    ff = [[[remote(hid[k % RING].at[core * X + back(x, d, X), pl.ds(0, own[k]), c], hid[k % RING].at[core * X + back(x, d, X), pl.ds(0, own[k]), c],
                   f_s.at[k % 2, b, d - 1], p_r.at[k % RING], partner) for d in range(1, X)]
           for b, c in enumerate(cols_of)] for k in range(K)]
    yy = [[[remote(ysend.at[k % 2, d - 1, :, pl.ds(0, ns[k]), pl.ds(s, w)], yrecv[k].at[d - 1, :, :, pl.ds(s, w)],
                   y_s.at[k % 2, t, d - 1], y_r.at[k, t, d - 1], ydev(d)) for d in range(1, Ry)]
           for t, (s, w) in enumerate(dblk)] for k in range(K)]
    zz = [[[remote(zsend.at[k % 2, d - 1, pl.ds(0, ns[k]), pl.ds(s, w)], zrecv[k].at[d - 1, :, pl.ds(s, w)],
                   z_s.at[k % 2, t, d - 1], z_r.at[k, t], zdev(d)) for d in range(1, Rz)]
           for t, (s, w) in enumerate(dblk)] for k in range(K)]

    def stage_g(k, b):
        if b == 0:
            with sc(f"w_ay{k}"):
                for c in ay_all[k]:
                    c.wait_recv()
        if k >= 1:
            dd[k - 1][b].wait_send()
        hy, half = Ry // 2, T[k] // 2
        cols = cols_of[b]
        repack = ns[k] < LARGE

        def operand():
            return jnp.concatenate([acts[k][pl.ds(core * hy, hy)].reshape(half, Dl),
                                    acts[k][pl.ds((1 - core) * hy, hy)].reshape(half, Dl)], axis=0)
        if repack and b == 0:
            with sc(f"pack{k}"):
                packed[...] = operand()

        def one(g, carry):
            lhs = jnp.concatenate([packed[...]] * 2, axis=0) if repack else operand()
            r = jnp.dot(lhs, wt[g, :, cols], preferred_element_type=F32)
            keep[k % 2, g, pl.ds(0, half), cols] = r[:half]
            dsend[g, pl.ds(0, half), cols] = r[half:T[k]]
            return carry
        with sc(f"G{k}_{b}"):
            lax.fori_loop(0, 2, one, 0)
        if k >= 1:
            pl.semaphore_wait(credit, 1)
        dd[k][b].start()

    def stage_x(k, b):
        with sc(f"w_dd{k}_{b}"):
            dd[k][b].wait_recv()
        if k >= 2:
            for c in xx[k - 2][b]:
                c.wait_send()
        o = own[k]
        for d in range(1, X):
            rows = pl.ds(pl.multiple_of(hop(x, d, X) * o, o), o)
            for g in range(2):
                def tile(cols, g=g, rows=rows, d=d):
                    xsend[k % 2, d - 1, g, pl.ds(0, o), cols] = (
                        keep[k % 2, g, rows, cols] + drecv[g, rows, cols]).astype(BF16)
                for_tiles(*fblk[b], tile)
            xx[k][b][d - 1].start()
        rows = pl.ds(pl.multiple_of(x * o, o), o)
        for g in range(2):
            def tile(cols, g=g):
                keep[k % 2, g, rows, cols] = keep[k % 2, g, rows, cols] + drecv[g, rows, cols]
            for_tiles(*fblk[b], tile)
        if k + 1 < K:
            pl.semaphore_signal(credit, inc=1, device_id=partner, device_id_type=MESH)

    def stage_s(k):
        o, n = own[k], ns[k]
        scales = []
        for i in range(nb):
            blk = pos * nb + i
            first = (lax.rem(blk, Rz) * Ry + blk // Rz) * tpr + offs[k]
            want = first + lax.broadcasted_iota(jnp.int32, (n, tok), 0)
            hit = lax.broadcasted_iota(jnp.int32, (n, tok), 1) == want
            scales.append(jnp.sum(jnp.where(hit, act_scale[...], 0.0), axis=1, keepdims=True))
        scale = jnp.concatenate(scales, axis=0)
        rows = pl.ds(pl.multiple_of(x * o, o), o)
        for b in range(NB):
            with sc(f"w_xx{k}_{b}"):
                for c in xx[k][b]:
                    c.wait_recv()

            def tile(cols):
                vals = []
                for g in range(2):
                    v = keep[k % 2, g, rows, cols]
                    for d in range(1, X):
                        v = v + xrecv[k % RING][d - 1, g, pl.ds(0, o), cols].astype(F32)
                    vals.append(v * scale * gu_scale[g:g + 1, cols])
                hid[k % RING][pos, pl.ds(0, o), cols] = (vals[0] / (1.0 + jnp.exp(-vals[0])) * vals[1]).astype(BF16)
            with sc(f"S{k}_{b}"):
                for_tiles(*fblk[b], tile)
            for c in hh[k][b]:
                c.start()
            hp[k][b].start()

    def stage_h(k, blocks=None):
        for b in range(NB) if blocks is None else blocks:
            with sc(f"w_hh{k}_{b}"):
                for c in hh[k][b]:
                    c.wait_recv()
            for c in ff[k][b]:
                c.start()

    def ready_d(k):
        if k == 0:
            with sc("w_down"):
                for i in range(nfull):
                    wcopy(2, i).wait()
                if tail:
                    wcopy(2, nfull, tail).wait()
        if k >= 2:
            for t in range(len(dblk)):
                for c in yy[k - 2][t]:
                    c.wait_send()
        with sc(f"w_ff{k}"):
            theirs = hid[k % RING].at[pl.ds((1 - core) * X, X), pl.ds(0, own[k])]
            remote(theirs, theirs, p_s.at[k % RING, 0], p_r.at[k % RING], partner).wait_recv()

    def after_d(k):
        for c in sum(ff[k], []):
            c.wait_send()

    def stage_d(k):
        ready_d(k)
        for t in range(len(dblk)):
            down_tile(k, t)
        after_d(k)

    def down_tile(k, t):
        n, per = ns[k], C // Ry
        s, w = dblk[t]
        with sc(f"D{k}_{t}"):
            lhs = [hid[k % RING][pl.ds(hop(y, d, Ry) * per, per), pl.ds(0, own[k])].reshape(T[k] // Ry, Fl)
                   for d in range(Ry)]
            lhs = jnp.concatenate(lhs * (LARGE // n), axis=0)
            r = jnp.dot(lhs, wdn[:, pl.ds(s, w)], preferred_element_type=F32)[:T[k]].reshape(Ry, Rz, n, w)
            opart[k % 2, :, pl.ds(0, n), pl.ds(s, w)] = r[0]
            for d in range(1, Ry):
                ysend[k % 2, d - 1, :, pl.ds(0, n), pl.ds(s, w)] = r[d].astype(BF16)
        for c in yy[k][t]:
            c.start()

    def stage_y(k, only=None):
        n = ns[k]
        for t, (s, w) in enumerate(dblk):
            if only is not None and t not in only:
                continue
            with sc(f"w_yy{k}_{t}"):
                for c in yy[k][t]:
                    c.wait_recv()
            if k >= 2:
                for c in zz[k - 2][t]:
                    c.wait_send()
            cols = pl.ds(s, w)
            for d in range(1, Rz + 1):
                zt = hop(z, d, Rz) if d < Rz else z
                v = opart[k % 2, zt, pl.ds(0, n), cols]
                for e in range(1, Ry):
                    v = v + yrecv[k][e - 1, zt, :, cols].astype(F32)
                if d < Rz:
                    zsend[k % 2, d - 1, pl.ds(0, n), cols] = v.astype(BF16)
                    zz[k][t][d - 1].start()
                else:
                    zown[k][:, cols] = v

    def stage_z(k):
        for t, (s, w) in enumerate(dblk):
            with sc(f"w_zz{k}_{t}"):
                cols = pl.ds(s, w)
                remote(zrecv[k].at[:, :, cols], zrecv[k].at[:, :, cols], z_s.at[k % 2, t, 0], z_r.at[k, t],
                       zdev(1)).wait_recv()
            v = zown[k][:, cols]
            for d in range(1, Rz):
                v = v + zrecv[k][d - 1, :, cols].astype(F32)
            out[offs[k]:offs[k] + ns[k], cols] = (v * down_scale[:, cols]).astype(BF16)

    order = [(0, i) for i in range(nfull + 1)] + [(1, i) for i in range(nfull + 1)]
    stops = [min(5 + 5 * d // 2, len(order)) for d in range(Rz - 1)] + [len(order)]
    done = 0
    for d, stop in enumerate(stops):
        for g in range(2):
            mine = [i for h, i in order[done:stop] if h == g]
            if mine:
                turns(g, mine[0], mine[-1] + 1)
        done = stop
        if d < Rz - 1:
            forward(0, d + 1)
            if d == min(1, Rz - 2) and K > 1:
                gather(1)

    def settle(k):
        for c in az[k] + sum(ay[k], []) + sum(hh[k], []) + hp[k]:
            c.wait_send()

    for c in inputs[1:]:
        c.wait()
    for it in range(K):
        late = it == 3
        for b in range(NB):
            stage_g(it, b)
            if b >= 1 and not late:
                stage_x(it, b - 1)
            if it + 1 < K:
                for d in range(1, Rz):
                    if min(d - 1, NB - 1) == b:
                        forward(it + 1, d)
            if b == min(2, NB - 1) and it + 2 < K:
                gather(it + 2)
        if late:
            stage_s(it - 1)
        for b in range(0 if late else NB - 1, NB):
            stage_x(it, b)
        if it >= 3:
            stage_y(it - 3)
        if it >= 1 and not late:
            stage_s(it - 1)
        if it >= 2:
            stage_h(it - 2)
            stage_d(it - 2)
        if it >= 3:
            settle(it - 3)
        if it >= 4:
            stage_z(it - 4)
    if K >= 3:
        settle(K - 3)
    if K >= 2:
        for c in sum(xx[K - 2], []):
            c.wait_send()
    stage_s(K - 1)
    if K >= 2:
        stage_h(K - 2, range(NB - 1))
    if K >= 3:
        stage_y(K - 3, (0,))
    if K >= 2:
        stage_h(K - 2, (NB - 1,))
        ready_d(K - 2)
    for t in range(len(dblk)):
        if K >= 2:
            down_tile(K - 2, t)
        if K >= 3 and t + 1 < len(dblk):
            stage_y(K - 3, (t + 1,))
        if t == 0:
            stage_h(K - 1)
    ready_d(K - 1)
    for t in range(len(dblk)):
        down_tile(K - 1, t)
    if K >= 2:
        stage_y(K - 2)
    stage_y(K - 1)
    for c in dd[K - 1] + sum(xx[K - 1], []):
        c.wait_send()
    for k in range(max(K - 2, 0), K):
        after_d(k)
        settle(k)
    if K >= 4:
        stage_z(K - 4)
    for k in range(max(K - 2, 0), K):
        for c in sum(yy[k], []):
            c.wait_send()
    for k in range(max(K - 3, 0), K):
        stage_z(k)
    with sc("end"):
        for k in range(max(K - 2, 0), K):
            for c in sum(zz[k], []):
                c.wait_send()


def solution(mesh):
    R, C = mesh.shape["row"], mesh.shape["col"]
    X = C // 2
    Ry = max(d for d in range(1, R + 1) if R % d == 0 and d * d <= R)
    Rz = R // Ry

    def body(act, act_scale, gu, gu_scale, down, down_scale):
        tpr, Dl = act.shape
        Fl = gu.shape[2]
        ns = chunks_of(tpr)
        K, n = len(ns), max(ns)
        T = R * n
        own = T // C
        NB, ND, NT = len(blocks_of(Fl)), len(tiles_of(Dl)), len(pieces(Fl, TTILE))
        vmem = pl.BlockSpec(memory_space=pltpu.VMEM)
        hbm = pl.BlockSpec(memory_space=pl.ANY)
        dma = pltpu.SemaphoreType.DMA
        scratch = [
            pltpu.VMEM((2, Dl, Fl), BF16),
            pltpu.VMEM((Fl, Dl), BF16),
            pltpu.VMEM((2, 2, T // 2, Fl), F32),
            pltpu.VMEM((2, T // 2, Fl), F32),
            pltpu.VMEM((2, T // 2, Fl), F32),
            pltpu.VMEM((2, X - 1, 2, own, Fl), BF16),
            pltpu.VMEM((2, Rz, n, Dl), F32),
            pltpu.VMEM((2, Ry - 1, Rz, n, Dl), BF16),
            pltpu.VMEM((2, Rz - 1, n, Dl), BF16),
            pltpu.VMEM((R * SMALL, Dl), BF16),
            pltpu.VMEM(act.shape, BF16),
            pltpu.VMEM((1, act_scale.shape[0]), F32),
            pltpu.VMEM(gu_scale.shape, F32),
            pltpu.VMEM((1, Dl), F32),
            dma((4,)),
            *[pltpu.VMEM((Ry, Rz, m, Dl), BF16) for m in ns],
            *[pltpu.VMEM((X - 1, 2, own, Fl), BF16)] * RING,
            *[pltpu.VMEM((C, own, Fl), BF16)] * RING,
            *[pltpu.VMEM((Ry - 1, Rz, m, Dl), BF16) for m in ns],
            *[pltpu.VMEM((Rz - 1, m, Dl), BF16) for m in ns],
            *[pltpu.VMEM((m, Dl), F32) for m in ns],
            dma((NT,)),
            dma((K, Rz - 1)), dma((K, Rz - 1)),
            dma((K, Rz, Ry - 1)), dma((K, Ry - 1)),
            dma((NB,)), dma((NB,)),
            dma((2, NB, X - 1)), dma((RING, NB, X - 1)),
            dma((RING, NB, X - 1)), dma((RING, NB, X - 1)),
            dma((RING, NB)), dma((RING,)),
            dma((2, NB, X - 1)),
            dma((2, ND, Ry - 1)), dma((K, ND, Ry - 1)),
            dma((2, ND, Rz - 1)), dma((K, ND)),
            pltpu.SemaphoreType.REGULAR,
        ]
        return pl.pallas_call(
            functools.partial(kernel, ns, Rz, Ry, X),
            out_shape=pltpu.VMEM((tpr, Dl), BF16),
            in_specs=[hbm] * 6,
            out_specs=vmem,
            scratch_shapes=scratch,
            compiler_params=pltpu.CompilerParams(
                collective_id=0, has_side_effects=True, vmem_limit_bytes=67043328 - 2 * tpr * Dl * 2
            ),
        )(act, act_scale.reshape(1, -1), jnp.swapaxes(gu, 1, 2), gu_scale, down, down_scale.reshape(1, Dl))

    in_specs = (P("row", "col"), P(), P(None, "col", "row"), P(None, "row"), P("row", "col"), P("col"))
    return jax.shard_map(body, mesh=mesh, in_specs=in_specs, out_specs=P("row", "col"), check_vma=False)
```
